32 devices in a mesh: seq: 2 (over x), tp: 4 (over z), pp: 4 (over y, core).
Axes of the slice: x: 2, y: 2, z: 4, core: 2. Of those that a mesh axis runs over, the one named last changes fastest.
Arguments:
- queries: bfloat16 [4, 384, 8192], P('pp', 'seq', 'tp'), may hold values from -40 to 40
- keys: bfloat16 [4, 384, 1024], P('pp', 'seq', 'tp'), may hold values from -16 to 16
- values: bfloat16 [4, 384, 1024], P('pp', 'seq', 'tp'), may hold values from -6 to 6
- doc_lengths: int32 [4, 8], P('pp'), may hold values from 1 to 288, 384 in all within a row
- resid: bfloat16 [4, 384, 5120], P('pp', 'seq', 'tp'), may hold values from -8 to 8
- ffn_gain: float32 [4, 5120], P('pp'), may hold values from 0.1 to 1.9
- w_gate: bfloat16 [4, 5120, 12800], P('pp', None, ('seq', 'tp')), may hold values from -0.078125 to 0.078125
- w_up: bfloat16 [4, 5120, 12800], P('pp', None, ('seq', 'tp')), may hold values from -0.078125 to 0.078125
- w_down: bfloat16 [4, 12800, 5120], P('pp', 'seq', 'tp'), may hold values from -0.0546875 to 0.0546875
- kv_gain: float32 [4, 5120], P('pp'), may hold values from 0.1 to 1.9
- key_value_weight: bfloat16 [4, 5120, 2048], P('pp', 'tp'), may hold values from -0.078125 to 0.078125
- k_gain: float32 [4, 128], P('pp'), may hold values from 0.1 to 1.9
Outputs:
- attn_out: bfloat16 [4, 384, 8192], P('pp', 'seq', 'tp')
- layer_out: bfloat16 [4, 384, 5120], P('pp', 'seq', 'tp')
- kv_next: bfloat16 [4, 384, 2048], P('pp', 'seq', 'tp')
The draws below stay inside these ranges and needn't reach their ends.
All inputs are finite; a program needn't handle non-finite values.
Results may differ from the reference program's by a relative error of at most 0.019.
Values may be sent and summed in bfloat16 or wider, within the bound.
A program may use at most 192 MiB of HBM per device.

```python
import math
import jax
import jax.numpy as jnp
import numpy as np
from jax import lax

MODEL_WIDTH = 5120
FF = 12800
QUERY_HEADS = 64
KEY_VALUE_HEADS = 8
HEAD_SIZE = 128
DOCS = 8
BATCH_TOKENS = 384
RELAY_SECTIONS = 4
DOC_MOST = 288


def query_key_pair(key):
    random_keys = jax.random.split(jax.random.fold_in(key, 4242), 2)
    query_bulk = 1.6 * jnp.clip(jax.random.normal(random_keys[0], (RELAY_SECTIONS, BATCH_TOKENS, QUERY_HEADS, HEAD_SIZE), jnp.float32), -6.0, 6.0)
    key_mass = jnp.clip(jax.random.normal(random_keys[1], (RELAY_SECTIONS, BATCH_TOKENS, KEY_VALUE_HEADS, HEAD_SIZE), jnp.float32), -6.0, 6.0)
    query_final = jnp.clip(query_bulk, -40.0, 40.0).reshape(RELAY_SECTIONS, BATCH_TOKENS, QUERY_HEADS * HEAD_SIZE)
    key_ending = jnp.clip(key_mass, -16.0, 16.0).reshape(RELAY_SECTIONS, BATCH_TOKENS, KEY_VALUE_HEADS * HEAD_SIZE)
    return (query_final, key_ending)


def draw_queries(key, part):
    return query_key_pair(key)[0].astype(jnp.bfloat16)


def draw_keys(key, part):
    return query_key_pair(key)[1].astype(jnp.bfloat16)


def draw_resid(key, part):
    random_keys = jax.random.split(jax.random.fold_in(key, 77), 3)
    row_scales = jnp.exp(jax.random.uniform(random_keys[0], (RELAY_SECTIONS, BATCH_TOKENS, 1), jnp.float32, math.log(0.3), math.log(3.0)))
    rising = (1.0 + 2.0 * jnp.arange(MODEL_WIDTH, dtype=jnp.float32) / (MODEL_WIDTH - 1)) / 2.0
    col_scales = jnp.exp(jax.random.uniform(random_keys[1], (RELAY_SECTIONS, 1, MODEL_WIDTH), jnp.float32, math.log(0.3), math.log(3.0))) * rising[None, None, :]
    base_values = jax.random.normal(random_keys[2], (RELAY_SECTIONS, BATCH_TOKENS, MODEL_WIDTH), jnp.float32)
    return jnp.clip(0.5 * base_values * row_scales * col_scales, -8.0, 8.0).astype(jnp.bfloat16)


def block_levels(key, shape, cuts, low, top_value):
    def one(position, blocks):
        heights = jax.random.uniform(jax.random.fold_in(jax.random.fold_in(key, 6), position), (blocks,), jnp.float32, low / len(cuts), top_value / len(cuts))
        return jnp.repeat(jnp.exp(heights), shape[position] // blocks).reshape((-1,) + (1,) * (len(shape) - position - 1))

    factor_of = one(*cuts[0])
    for cut in cuts[1:]:
        factor_of = factor_of * one(*cut)
    return factor_of


def length_profile(number_of, total, most, slope):
    portions = [(1 << 20) // math.isqrt(standing ** slope) + 1 for standing in range(2, number_of + 1)]
    spare, given = total - most - (number_of - 1), [1] * (number_of - 1)
    while spare > 0:
        candidates = [i for i in range(number_of - 1) if given[i] < most]
        pool, left = sum([portions[i] for i in candidates]), spare
        for i in candidates:
            addition = min(most - given[i], max(1, left * portions[i] // pool), spare)
            given[i] = given[i] + addition
            spare = spare - addition
    return np.array([most] + given)


def uneven(key, count, total, most, slope):
    if count == 2:
        one = jax.random.randint(key, (), max(1, total - most), min(most, total - 1) + 1)
        return jnp.stack([one, total - one])
    tallies = jnp.asarray(length_profile(count, total, most, slope), jnp.int32)
    pairs = (count - 1) // 2
    giver, sink = tallies[1:1 + 2 * pairs:2], tallies[2:2 + 2 * pairs:2]
    margin = jnp.minimum(giver - 1, most - sink)
    passed = jax.random.randint(jax.random.fold_in(key, 1), (pairs,), 0, 1 << 20) % (margin + 1)
    tallies = tallies.at[1:1 + 2 * pairs:2].set(giver - passed).at[2:2 + 2 * pairs:2].set(sink + passed)
    return tallies[jax.random.permutation(jax.random.fold_in(key, 2), count)]


def gaussian(own_key, extent, width, most, cuts=(), kind=jnp.bfloat16):
    values = jax.random.normal(own_key, extent, jnp.float32) * width
    if len(cuts) > 0:
        values = block_levels(own_key, extent, cuts, -0.22, 0.18) * values
    return jnp.clip(values, min=-most, max=most).astype(kind)


def setup_inputs(seed: int = 0) -> dict:
    key_of = jax.random.split(jax.random.key(seed), 13)
    return {
        "queries": draw_queries(jax.random.fold_in(key_of[12], 71), 0),
        "keys": draw_keys(jax.random.fold_in(key_of[12], 71), 0),
        "values": gaussian(key_of[2], (RELAY_SECTIONS, BATCH_TOKENS, KEY_VALUE_HEADS * HEAD_SIZE), 1.0, 6.0, ((0, 4), (1, 2), (2, 4))),
        "doc_lengths": jax.vmap(lambda own: uneven(own, DOCS, BATCH_TOKENS, DOC_MOST, 2))(jax.random.split(key_of[3], RELAY_SECTIONS)).reshape((RELAY_SECTIONS, DOCS)).astype(jnp.int32),
        "resid": draw_resid(jax.random.fold_in(key_of[12], 71), 0),
        "ffn_gain": jnp.clip(1.0 + 0.18 * jax.random.normal(key_of[5], (RELAY_SECTIONS, MODEL_WIDTH), jnp.float32), 0.1, 1.9),
        "w_gate": gaussian(key_of[6], (RELAY_SECTIONS, MODEL_WIDTH, FF), MODEL_WIDTH ** -0.5, 0.078125, ((0, 4), (2, 8))),
        "w_up": gaussian(key_of[7], (RELAY_SECTIONS, MODEL_WIDTH, FF), MODEL_WIDTH ** -0.5, 0.078125, ((0, 4), (2, 8))),
        "w_down": gaussian(key_of[8], (RELAY_SECTIONS, FF, MODEL_WIDTH), FF ** -0.5, 0.0546875, ((0, 4), (1, 2), (2, 4))),
        "kv_gain": jnp.clip(1.0 + 0.18 * jax.random.normal(key_of[9], (RELAY_SECTIONS, MODEL_WIDTH), jnp.float32), 0.1, 1.9),
        "key_value_weight": gaussian(key_of[10], (RELAY_SECTIONS, MODEL_WIDTH, 2 * KEY_VALUE_HEADS * HEAD_SIZE), MODEL_WIDTH ** -0.5, 0.078125, ((0, 4), (1, 4))),
        "k_gain": jnp.clip(1.0 + 0.18 * jax.random.normal(key_of[11], (RELAY_SECTIONS, HEAD_SIZE), jnp.float32), 0.1, 1.9),
    }


epsilon = 1e-06
negative = -1e+30

def document_ids(lengths, tally_count):
    bounds = jnp.cumsum(lengths).astype(jnp.int32)
    places = jnp.arange(tally_count, dtype=jnp.int32)
    return lax.optimization_barrier(jnp.sum((places[:, None] >= bounds[None, :]).astype(jnp.int32), axis=1))

def attend_group(query_group, key_group, value_group, visible):
    scores = jnp.einsum('tgd,sd->gts', query_group.astype(jnp.float32), key_group.astype(jnp.float32)) / math.sqrt(HEAD_SIZE)
    masked = jnp.where(visible[None], scores, negative)
    row_peak = lax.optimization_barrier(jnp.max(masked, axis=2, keepdims=True))
    exponent = jnp.where(visible[None], jnp.exp(masked - row_peak), 0.0)
    row_total = lax.optimization_barrier(jnp.sum(exponent, axis=2))
    weights = lax.optimization_barrier(exponent.astype(jnp.bfloat16)).astype(jnp.float32)
    mixed = jnp.einsum('gts,sd->tgd', weights, value_group.astype(jnp.float32))
    return mixed / jnp.transpose(row_total)[:, :, None]

def attend_segment(operands):
    queries, keys, values, lengths = operands
    tally_count = queries.shape[0]
    docs = document_ids(lengths, tally_count)
    places = jnp.arange(tally_count, dtype=jnp.int32)
    visible = (docs[:, None] == docs[None, :]) & (places[None, :] <= places[:, None])
    query_per_head = jnp.moveaxis(queries.reshape(tally_count, KEY_VALUE_HEADS, QUERY_HEADS // KEY_VALUE_HEADS, HEAD_SIZE), 1, 0)
    key_per_head = jnp.moveaxis(keys.reshape(tally_count, KEY_VALUE_HEADS, HEAD_SIZE), 1, 0)
    value_per_head = jnp.moveaxis(values.reshape(tally_count, KEY_VALUE_HEADS, HEAD_SIZE), 1, 0)
    mixed = lax.map(lambda triple: attend_group(triple[0], triple[1], triple[2], visible), (query_per_head, key_per_head, value_per_head))
    return jnp.moveaxis(mixed, 0, 1).reshape(tally_count, QUERY_HEADS * HEAD_SIZE).astype(jnp.bfloat16)

def ffn_segment(operands):
    resid, gain, gate_weight, up_weight, down_weight = operands
    wide = resid.astype(jnp.float32)
    inverse = lax.rsqrt(lax.optimization_barrier(jnp.mean(wide * wide, axis=-1, keepdims=True)) + epsilon)
    normed = (wide * inverse * gain[None, :]).astype(jnp.bfloat16)
    gate_total = jnp.dot(normed, gate_weight, preferred_element_type=jnp.float32)
    up_total = jnp.dot(normed, up_weight, preferred_element_type=jnp.float32)
    hidden = (jax.nn.silu(gate_total) * up_total).astype(jnp.bfloat16)
    return (wide + jnp.dot(hidden, down_weight, preferred_element_type=jnp.float32)).astype(jnp.bfloat16)

def kv_segment(operands):
    incoming, gain, kv_weight, key_gain = operands
    tally_count = incoming.shape[0]
    wide = incoming.astype(jnp.float32)
    inverse = lax.rsqrt(lax.optimization_barrier(jnp.mean(wide * wide, axis=-1, keepdims=True)) + epsilon)
    kv_input = (wide * inverse * gain[None, :]).astype(jnp.bfloat16)
    mapped_rows = jnp.dot(kv_input, kv_weight, preferred_element_type=jnp.float32)
    key_portion = mapped_rows[:, :KEY_VALUE_HEADS * HEAD_SIZE].reshape(tally_count, KEY_VALUE_HEADS, HEAD_SIZE)
    key_square = lax.optimization_barrier(jnp.mean(key_portion * key_portion, axis=2, keepdims=True))
    key_after_norm = key_portion * lax.rsqrt(key_square + epsilon) * key_gain[None, None, :]
    combined = jnp.concatenate([key_after_norm.reshape(tally_count, KEY_VALUE_HEADS * HEAD_SIZE), mapped_rows[:, KEY_VALUE_HEADS * HEAD_SIZE:]], axis=1)
    return combined.astype(jnp.bfloat16)

def reference(queries, keys, values, doc_lengths, resid, ffn_gain, w_gate, w_up, w_down, kv_gain, key_value_weight, k_gain):
    attn_out = lax.map(attend_segment, (queries, keys, values, doc_lengths))
    layer_out = lax.map(ffn_segment, (resid, ffn_gain, w_gate, w_up, w_down))
    incoming = jnp.roll(layer_out, 1, axis=0)
    kv_next = lax.map(kv_segment, (incoming, kv_gain, key_value_weight, k_gain))
    return (attn_out, layer_out, kv_next)
```

```python
import math

import jax
import jax.numpy as jnp
from jax import lax
from jax.sharding import PartitionSpec as P

MODEL_WIDTH = 5120
QUERY_HEADS = 64
KEY_VALUE_HEADS = 8
HEAD_SIZE = 128


epsilon = 1e-06
negative = -1e30


def passed_along(block, axis, distance):
    count = lax.axis_size(axis)
    return lax.ppermute(block, axis, [(i, (i + distance) % count) for i in range(count)])


def passed_where(block, distance, places):
    seq_count = lax.axis_size("seq")
    tp_count = lax.axis_size("tp")
    route = [
        (s * tp_count + t, ((s + distance) % seq_count) * tp_count + t)
        for s in range(seq_count)
        for t in places
    ]
    return lax.ppermute(block, ("seq", "tp"), route)


def line_gather(block):
    count = lax.axis_size("tp")
    slots = {0: block}
    for k in range(1, count):
        slots[-k] = lax.ppermute(
            slots[1 - k], "tp", [(i, i + 1) for i in range(k - 1, count - 1)]
        )
        slots[k] = lax.ppermute(
            slots[k - 1], "tp", [(i, i - 1) for i in range(1, count - k + 1)]
        )
    return slots


def valid_places(offset, count):
    return [t for t in range(count) if 0 <= t + offset < count]


def pick(slots, offsets, tp_rank):
    picked = slots[offsets[0]]
    for t in range(1, len(offsets)):
        if offsets[t] != offsets[t - 1] or len(set(offsets)) > 1:
            picked = jnp.where(tp_rank == t, slots[offsets[t]], picked)
    return picked


def arrival_order(count):
    table = []
    for t in range(count):
        order = [0]
        for k in range(1, count):
            order += [d for d in (-k, k) if 0 <= t + d < count]
        table.append(order)
    return table


def document_ids(places, bounds):
    return jnp.sum((places[:, None] >= bounds[None, :]).astype(jnp.int32), axis=1)


def seq_gather(block):
    count = lax.axis_size("seq")
    rank = lax.axis_index("seq")
    rows = block.shape[0]
    whole = jnp.zeros((count * rows, block.shape[1]), block.dtype)
    for k in range(count):
        part = block if k == 0 else passed_along(block, "seq", k)
        whole = lax.dynamic_update_slice_in_dim(whole, part, lax.rem(rank - k + count, count) * rows, 0)
    return whole


def attend_rows(query_rows, query_places, keys_local, values_local, lengths):
    bounds = jnp.cumsum(lengths)
    query_docs = document_ids(query_places, bounds)
    row_count = query_rows.shape[0]
    kv_heads = keys_local.shape[1] // HEAD_SIZE
    group_width = QUERY_HEADS // KEY_VALUE_HEADS
    query_four = query_rows.reshape(row_count, kv_heads, group_width, HEAD_SIZE)
    inv_root = 1.0 / math.sqrt(HEAD_SIZE)
    key_piece = seq_gather(keys_local)
    value_piece = seq_gather(values_local)
    key_count = key_piece.shape[0]

    key_places = jnp.arange(key_count, dtype=jnp.int32)
    key_docs = document_ids(key_places, bounds)
    visible = (query_docs[:, None] == key_docs[None, :]) & (
        key_places[None, :] <= query_places[:, None]
    )
    scores = (
        jnp.einsum(
            "rkgd,nkd->kgrn",
            query_four,
            key_piece.reshape(key_count, kv_heads, HEAD_SIZE),
            preferred_element_type=jnp.float32,
        )
        * inv_root
    )
    masked = jnp.where(visible, scores, negative)
    row_max = jnp.max(masked, axis=3)
    exponent = jnp.where(visible, jnp.exp(masked - row_max[..., None]), 0.0)
    running_sum = jnp.sum(exponent, axis=3)
    weighted = jnp.einsum(
        "kgrn,nkd->kgrd",
        exponent.astype(jnp.bfloat16),
        value_piece.reshape(key_count, kv_heads, HEAD_SIZE),
        preferred_element_type=jnp.float32,
    )
    mixed = weighted / running_sum[..., None]
    return (
        jnp.transpose(mixed, (2, 0, 1, 3))
        .reshape(row_count, kv_heads * group_width * HEAD_SIZE)
        .astype(jnp.bfloat16)
    )


def body(
    queries,
    keys,
    values,
    doc_lengths,
    resid,
    ffn_gain,
    w_gate,
    w_up,
    w_down,
    kv_gain,
    key_value_weight,
    k_gain,
):
    seq_count = lax.axis_size("seq")
    seq_rank = lax.axis_index("seq")
    tp_count = lax.axis_size("tp")
    tp_rank = lax.axis_index("tp")
    tok_rows = queries.shape[1]
    lengths = doc_lengths[0]
    query_local = queries[0]
    query_places = seq_rank * tok_rows + jnp.arange(tok_rows, dtype=jnp.int32)
    attended = attend_rows(query_local, query_places, keys[0], values[0], lengths)
    resid_local = resid[0]
    wide = resid_local.astype(jnp.float32)
    features = resid_local.shape[1]
    hidden_local = w_gate.shape[2]
    slots = line_gather(resid_local)
    groups = [slots]
    for k in range(1, seq_count):
        groups.append(
            {d: passed_where(slots[d], k, valid_places(d, tp_count)) for d in sorted(slots, key=abs)}
        )
    gain = ffn_gain[0]
    table = arrival_order(tp_count)
    down_weight = w_down[0]
    totals = []
    for group in groups:
        pieces = [
            pick(group, [j - t for t in range(tp_count)], tp_rank).astype(jnp.float32)
            for j in range(tp_count)
        ]
        squares = sum(jnp.sum(piece * piece, axis=1) for piece in pieces)
        inverse = lax.rsqrt(squares / MODEL_WIDTH + epsilon)
        normed = jnp.concatenate(
            [
                (
                    pieces[j] * inverse[:, None] * gain[None, j * features : (j + 1) * features]
                ).astype(jnp.bfloat16)
                for j in range(tp_count)
            ],
            axis=1,
        )
        gate_total = jnp.dot(normed, w_gate[0], preferred_element_type=jnp.float32)
        up_total = jnp.dot(normed, w_up[0], preferred_element_type=jnp.float32)
        hidden = (jax.nn.silu(gate_total) * up_total).astype(jnp.bfloat16)
        hidden_slots = line_gather(hidden)
        total = None
        for m in range(tp_count):
            offsets = [table[t][m] for t in range(tp_count)]
            block = pick(hidden_slots, offsets, tp_rank)
            place = tp_rank + jnp.asarray(offsets, jnp.int32)[tp_rank]
            rows = lax.dynamic_slice_in_dim(down_weight, place * hidden_local, hidden_local)
            term = jnp.dot(block, rows, preferred_element_type=jnp.float32)
            total = term if total is None else total + term
        totals.append(total)
    update_rows = totals[0]
    for k in range(1, seq_count):
        update_rows = update_rows + passed_along(
            totals[k].astype(jnp.bfloat16), "seq", -k
        ).astype(jnp.float32)
    layer_local = (wide + update_rows).astype(jnp.bfloat16)
    incoming = passed_along(layer_local, "pp", 1)
    incoming_wide = incoming.astype(jnp.float32)
    own_square = jnp.sum(incoming_wide * incoming_wide, axis=1)
    incoming_total = own_square
    for k in range(1, tp_count):
        incoming_total = incoming_total + passed_along(own_square, "tp", k)
    scale_rows = lax.rsqrt(incoming_total / MODEL_WIDTH + epsilon)
    kv_gain_part = lax.dynamic_slice_in_dim(kv_gain[0], tp_rank * features, features)
    kv_input = (incoming_wide * kv_gain_part[None, :]).astype(jnp.bfloat16)
    kv_weight = key_value_weight[0]
    span = kv_weight.shape[1] // tp_count
    mapped_rows = jnp.dot(kv_input, kv_weight, preferred_element_type=jnp.float32)
    kv_span = lax.dynamic_slice_in_dim(mapped_rows, tp_rank * span, span, 1)
    mapped_bits = mapped_rows.astype(jnp.bfloat16)
    for k in range(1, tp_count):
        part = lax.dynamic_slice_in_dim(mapped_bits, lax.rem(tp_rank + k, tp_count) * span, span, 1)
        kv_span = kv_span + passed_along(part, "tp", k).astype(jnp.float32)
    kv_span = kv_span * scale_rows[:, None]
    span_width = kv_span.shape[1]
    heads_here = span_width // HEAD_SIZE
    divide_heads = kv_span.reshape(tok_rows, heads_here, HEAD_SIZE)
    mean_square = jnp.mean(divide_heads * divide_heads, axis=2, keepdims=True)
    norm_applied = divide_heads * lax.rsqrt(mean_square + epsilon) * k_gain[0][None, None, :]
    head_index_list = tp_rank * heads_here + jnp.arange(heads_here, dtype=jnp.int32)
    kv_result = (
        jnp.where((head_index_list < KEY_VALUE_HEADS)[None, :, None], norm_applied, divide_heads)
        .reshape(tok_rows, span_width)
        .astype(jnp.bfloat16)
    )
    return (attended[None], layer_local[None], kv_result[None])


def solution(mesh):
    placed = (
        P("pp", "seq", "tp"),
        P("pp", "seq", "tp"),
        P("pp", "seq", "tp"),
        P("pp", None),
        P("pp", "seq", "tp"),
        P("pp", None),
        P("pp", None, ("seq", "tp")),
        P("pp", None, ("seq", "tp")),
        P("pp", "seq", "tp"),
        P("pp", None),
        P("pp", "tp", None),
        P("pp", None),
    )
    return jax.shard_map(
        body,
        mesh=mesh,
        in_specs=placed,
        out_specs=(P("pp", "seq", "tp"), P("pp", "seq", "tp"), P("pp", "seq", "tp")),
        check_vma=False,
    )
```
